32 devices in a mesh: row: 8 (over z, x), col: 4 (over y, core).
Axes of the slice: x: 2, y: 2, z: 4, core: 2. Of those that a mesh axis runs over, the one named last changes fastest.
Arguments:
- prior_scores: float32 [12288, 12288], P('row', 'col'), may hold values from 0.001 to 10
- tiles_first: bfloat16 [96, 5, 128, 128], P('row'), may hold values from 0 to 1, as said below
- columns_first: int32 [96, 5], P('row'), may hold values from 0 to 95, as said below
- tiles_second: bfloat16 [96, 5, 128, 128], P('col'), may hold values from 0 to 1, as said below
- columns_second: int32 [96, 5], P('col'), may hold values from 0 to 95, as said below
Outputs:
- alignment: float32 [12288, 12288], P('row', 'col')
The draws below stay inside these ranges and needn't reach their ends.
Inputs may be any that keep to these rules, and one draw needn't show every extreme that they name: `tiles_first`: in every block row, the block in the first slot has entries of 0.5 or more on its diagonal. `tiles_second`: in every block row, the block in the first slot has entries of 0.5 or more on its diagonal. `columns_first`: each block row lists 5 different block columns. `columns_second`: each block row lists 5 different block columns.
All inputs are finite; a program needn't handle non-finite values.
Results may differ from the reference program's by a relative error of at most 0.0004.
The reference program's roundings to bfloat16 on the way count: a program that leaves them out, or rounds other values in their place, can miss the bound.
Values may be sent and summed in bfloat16 or wider, within the bound.
A program may use at most 192 MiB of HBM per device.

```python
import jax
import jax.numpy as jnp
from jax import lax

NODES_A = 12288
NODES_B = 12288
TILE = 128
SLOTS = 5
ITERS = 2


weight_span = 13.815510557964274


log_ten = 2.302585092994046


def tile_draw(key, block_count):
    tile_shape = (block_count, SLOTS, TILE, TILE)
    keep_key, level_key, extra_key, diagonal_key = jax.random.split(key, 4)
    kept_mask = jax.random.randint(keep_key, tile_shape, 0, 3) == 0
    level_draw = jax.random.uniform(level_key, tile_shape, dtype=jnp.float32)
    values = jnp.where(kept_mask, jnp.exp((level_draw - 1.0) * weight_span), 0.0)
    diagonal = jax.random.uniform(diagonal_key, (block_count, TILE), dtype=jnp.float32, minval=0.5, maxval=1.0)
    unit_matrix = jnp.eye(TILE, dtype=jnp.float32)
    first_slot = values[:, 0] * (1.0 - unit_matrix)[None] + diagonal[:, :, None] * unit_matrix[None]
    values = jnp.concatenate([first_slot[:, None], values[:, 1:]], axis=1)
    return values.astype(jnp.bfloat16)


def draw_tiles_first(key, part):
    return tile_draw(jax.random.fold_in(key, 11), NODES_A // TILE)


def draw_tiles_second(key, part):
    return tile_draw(jax.random.fold_in(key, 13), NODES_B // TILE)


def draw_prior_scores(key, part):
    first_key, second_key = jax.random.split(jax.random.fold_in(key, 19))
    level_draw = jax.random.uniform(first_key, (NODES_A, NODES_B), dtype=jnp.float32)
    return jnp.exp((4.0 * level_draw - 3.0) * log_ten)


def draw_columns_first(key, part):
    block_count = NODES_A // TILE
    key_list = jax.random.split(key, block_count)
    return jax.vmap(lambda single: jax.random.permutation(single, block_count)[:SLOTS])(key_list).astype(jnp.int32)


def draw_columns_second(key, part):
    block_count = NODES_B // TILE
    key_list = jax.random.split(jax.random.fold_in(key, 7), block_count)
    return jax.vmap(lambda single: jax.random.permutation(single, block_count)[:SLOTS])(key_list).astype(jnp.int32)


def setup_inputs(seed: int = 0) -> dict:
    streams_of = jax.random.split(jax.random.key(seed), 6)
    return {
        "prior_scores": draw_prior_scores(jax.random.fold_in(streams_of[5], 71), 0),
        "tiles_first": draw_tiles_first(jax.random.fold_in(streams_of[5], 71), 0),
        "columns_first": draw_columns_first(jax.random.fold_in(streams_of[5], 71), 0),
        "tiles_second": draw_tiles_second(jax.random.fold_in(streams_of[5], 71), 0),
        "columns_second": draw_columns_second(jax.random.fold_in(streams_of[5], 71), 0),
    }


mixing = 0.8


def second_product(current, tile_set, columns, inverse):
    node_count = current.shape[0]
    blocks = current.reshape(node_count, -1, TILE)

    def per_block(operands):
        tiles_here, columns_here = operands
        picked = jnp.take(blocks, columns_here.astype(jnp.int32), axis=1).reshape(node_count, SLOTS * TILE)
        weight = tiles_here.transpose(0, 2, 1).reshape(SLOTS * TILE, TILE)
        return jnp.dot(picked, weight, preferred_element_type=jnp.float32)

    result = lax.map(per_block, (tile_set, columns))
    result = result.transpose(1, 0, 2).reshape(node_count, -1) * inverse[None, :]
    return result.astype(jnp.bfloat16)


def first_product(mixed_rows, tile_set, columns, inverse):
    width_b = mixed_rows.shape[1]
    blocks = mixed_rows.reshape(-1, TILE, width_b)

    def per_block(operands):
        tiles_here, columns_here = operands
        picked = jnp.take(blocks, columns_here.astype(jnp.int32), axis=0).reshape(SLOTS * TILE, width_b)
        weight = tiles_here.transpose(1, 0, 2).reshape(TILE, SLOTS * TILE)
        return jnp.dot(weight, picked, preferred_element_type=jnp.float32)

    result = lax.map(per_block, (tile_set, columns))
    result = result.reshape(-1, width_b) * inverse[:, None]
    return result.astype(jnp.bfloat16)


def reference(prior_scores, tiles_first, columns_first, tiles_second, columns_second):
    inverse_first = 1.0 / jnp.sum(tiles_first, axis=(1, 3), dtype=jnp.float32).reshape(-1)
    inverse_second = 1.0 / jnp.sum(tiles_second, axis=(1, 3), dtype=jnp.float32).reshape(-1)
    current_state = prior_scores
    for iteration in range(ITERS):
        current = current_state.astype(jnp.bfloat16)
        mixed_rows = second_product(current, tiles_second, columns_second, inverse_second)
        propagated = first_product(mixed_rows, tiles_first, columns_first, inverse_first)
        updated = mixing * propagated.astype(jnp.float32) + (1.0 - mixing) * prior_scores
        current_state = updated / (jnp.sum(updated) / float(NODES_A * NODES_B))
    return current_state
```

```python
import functools

import jax
import jax.numpy as jnp
from jax import lax
from jax.experimental import pallas as pl
from jax.experimental.pallas import tpu as pltpu
from jax.sharding import PartitionSpec as P

ITERS = 2
mixing = 0.8
CHUNKS = 4
SUBS = 4
MESH = pl.DeviceIdType.MESH
VMEM_LIMIT = 60 * 1024 * 1024


def divisor(total, wanted, unit):
    for count in range(wanted, 0, -1):
        if total % (count * unit) == 0:
            return count
    return 1


def comm_kernel(tasks, row_count, col_count, *refs):
    count = len(tasks)
    sources, targets = refs[:count], refs[count : 2 * count]
    scratch = refs[2 * count :]
    me_row, me_col = lax.axis_index("row"), lax.axis_index("col")
    has_gather = any(task[0] == "gather" for task in tasks)
    has_swap = any(task[0] == "swap" for task in tasks)
    paired = col_count % 2 == 0
    stride = 2 if paired else 1
    partner = me_col + 1 - 2 * lax.rem(me_col, 2)

    barrier = pltpu.get_barrier_semaphore()
    greeted = 0
    if has_gather:
        for step in range(1, col_count):
            peer = lax.rem(me_col + step, col_count)
            pl.semaphore_signal(barrier, inc=1, device_id=(me_row, peer), device_id_type=MESH)
            greeted += 1
    if has_swap:
        for step in range(1, row_count):
            peer = lax.rem(me_row + step, row_count)
            pl.semaphore_signal(barrier, inc=1, device_id=(peer, me_col), device_id_type=MESH)
            greeted += 1
    pl.semaphore_wait(barrier, greeted)

    pending = []
    local = []
    forwards = []
    for index, task in enumerate(tasks):
        source, target = sources[index], targets[index]
        bounce, local_sem, send_sem, recv_sem, pair_send, pair_recv = scratch[6 * index : 6 * index + 6]
        if task[0] == "gather":
            rows = source.shape[0]
            subs = divisor(rows, SUBS, 16)
            size = rows // subs
            for sub in range(subs):
                span = pl.ds(sub * size, size)
                for hop in range(1, col_count // stride):
                    peer = lax.rem(me_col + stride * hop, col_count)
                    origin = lax.rem(me_col + col_count - stride * hop, col_count)
                    slot = (hop - 1) * subs + sub
                    copy = pltpu.make_async_remote_copy(
                        src_ref=source.at[span],
                        dst_ref=target.at[me_col, span],
                        send_sem=send_sem.at[slot],
                        recv_sem=recv_sem.at[slot],
                        device_id=(me_row, peer),
                        device_id_type=MESH,
                    )
                    copy.start()
                    forwards.append((copy, target, origin, span, slot, pair_send, pair_recv))
            if paired:
                copy = pltpu.make_async_remote_copy(
                    src_ref=source,
                    dst_ref=target.at[me_col],
                    send_sem=pair_send.at[0],
                    recv_sem=pair_recv.at[0],
                    device_id=(me_row, partner),
                    device_id_type=MESH,
                )
                copy.start()
                pending.append(copy)
            local.append((source, target.at[me_col], bounce, local_sem))
        else:
            start, size = task[1], task[2]
            span = pl.ds(start, size)
            for step in range(1, row_count):
                peer = lax.rem(me_row + step, row_count)
                copy = pltpu.make_async_remote_copy(
                    src_ref=source.at[peer, span],
                    dst_ref=target.at[me_row],
                    send_sem=send_sem.at[step - 1],
                    recv_sem=recv_sem.at[step - 1],
                    device_id=(peer, me_col),
                    device_id_type=MESH,
                )
                copy.start()
                pending.append(copy)
            local.append((source.at[me_row, span], target.at[me_row], bounce, local_sem))

    for here, there, bounce, sem in local:
        copy = pltpu.make_async_copy(here, bounce, sem)
        copy.start()
        copy.wait()
        copy = pltpu.make_async_copy(bounce, there, sem)
        copy.start()
        copy.wait()

    for copy, target, origin, span, slot, pair_send, pair_recv in forwards:
        copy.wait_recv()
        if paired:
            onward = pltpu.make_async_remote_copy(
                src_ref=target.at[origin, span],
                dst_ref=target.at[origin, span],
                send_sem=pair_send.at[1 + slot],
                recv_sem=pair_recv.at[1 + slot],
                device_id=(me_row, partner),
                device_id_type=MESH,
            )
            onward.start()
            pending.append(onward)
    for item in forwards:
        item[0].wait_send()
    for copy in pending:
        copy.wait()


def communicate(tasks, sources, ident):
    row_count, col_count = lax.axis_size("row"), lax.axis_size("col")
    outs, scratch = [], []
    for task, source in zip(tasks, sources):
        if task[0] == "gather":
            shape = (col_count,) + source.shape
            slots = col_count * SUBS
            block = source.shape
        else:
            shape = (row_count, task[2], source.shape[2])
            slots = row_count
            block = shape[1:]
        outs.append(jax.ShapeDtypeStruct(shape, source.dtype))
        scratch += [
            pltpu.VMEM(block, source.dtype),
            pltpu.SemaphoreType.DMA,
            pltpu.SemaphoreType.DMA((slots,)),
            pltpu.SemaphoreType.DMA((slots,)),
            pltpu.SemaphoreType.DMA((slots + 1,)),
            pltpu.SemaphoreType.DMA((slots + 1,)),
        ]
    return pl.pallas_call(
        functools.partial(comm_kernel, tasks, row_count, col_count),
        out_shape=outs,
        in_specs=[pl.BlockSpec(memory_space=pl.ANY)] * len(tasks),
        out_specs=[pl.BlockSpec(memory_space=pl.ANY)] * len(tasks),
        scratch_shapes=scratch,
        compiler_params=pltpu.CompilerParams(
            collective_id=ident, has_side_effects=True, vmem_limit_bytes=VMEM_LIMIT
        ),
        name=f"comm_{ident}",
    )(*sources)


def second_kernel(slots, per, cols_ref, x_ref, tile_ref, inv_ref, out_ref):
    tile = tile_ref.shape[2]
    shard = x_ref.shape[2] // tile

    @pl.loop(0, out_ref.shape[0])
    def _(group):
        for inner in range(per):
            j = group * per + inner
            total = None
            for s in range(slots):
                column = cols_ref[j * slots + s]
                owner = column // shard
                start = pl.multiple_of((column - owner * shard) * tile, tile)
                term = jnp.dot(
                    x_ref[owner, :, pl.ds(start, tile)], tile_ref[j, s], preferred_element_type=jnp.float32
                )
                total = term if total is None else total + term
            out_ref[group, :, inner * tile : (inner + 1) * tile] = (total * inv_ref[j]).astype(jnp.bfloat16)


def second_product(gathered, tiles, columns, inverse, groups):
    col_count, rows, width = gathered.shape
    blocks, slots, tile, _ = tiles.shape
    steps = divisor(rows, 2, 16)
    size = rows // steps
    return pl.pallas_call(
        functools.partial(second_kernel, slots, blocks // groups),
        out_shape=jax.ShapeDtypeStruct((groups, rows, width // groups), jnp.bfloat16),
        grid_spec=pltpu.PrefetchScalarGridSpec(
            num_scalar_prefetch=1,
            grid=(steps,),
            in_specs=[
                pl.BlockSpec((col_count, size, width), lambda i, c: (0, i, 0)),
                pl.BlockSpec(tiles.shape, lambda i, c: (0, 0, 0, 0)),
                pl.BlockSpec(inverse.shape, lambda i, c: (0, 0, 0)),
            ],
            out_specs=pl.BlockSpec((groups, size, width // groups), lambda i, c: (0, i, 0)),
        ),
        compiler_params=pltpu.CompilerParams(vmem_limit_bytes=VMEM_LIMIT),
        name="second_product",
    )(columns, gathered, tiles, inverse)


def first_kernel(slots, parts, cols_ref, tile_ref, *refs):
    pieces, (out_ref, sum_ref, slab, sems) = refs[:parts], refs[parts:]
    step = pl.program_id(0)
    per, tile = tile_ref.shape[0], tile_ref.shape[2]
    in_part = slab.shape[2] // tile

    @pl.when(step == 0)
    def _():
        copies = [pltpu.make_async_copy(piece, slab.at[k], sems.at[k]) for k, piece in enumerate(pieces)]
        for copy in copies:
            copy.start()
        for copy in copies:
            copy.wait()
        sum_ref[...] = jnp.zeros_like(sum_ref)

    for inner in range(per):
        total, weight = None, None
        for s in range(slots):
            column = cols_ref[(step * per + inner) * slots + s]
            owner = column // (in_part * parts)
            rest = column - owner * (in_part * parts)
            part = rest // in_part
            start = pl.multiple_of((rest - part * in_part) * tile, tile)
            block = tile_ref[inner, s]
            term = jnp.dot(block, slab[part, owner, pl.ds(start, tile), :], preferred_element_type=jnp.float32)
            total = term if total is None else total + term
            wide = block.astype(jnp.float32)
            weight = wide if weight is None else weight + wide
        inverse = 1.0 / jnp.sum(weight, axis=1, keepdims=True)
        result = (total * inverse).astype(jnp.bfloat16)
        out_ref[inner * tile : (inner + 1) * tile, :] = result
        sum_ref[...] += jnp.sum(result.astype(jnp.float32).reshape(-1, 8, result.shape[1]), axis=0)


def first_product(pieces, tiles, columns):
    owners, size, width = pieces[0].shape
    blocks, slots, tile, _ = tiles.shape
    per = 4 if blocks % 4 == 0 else 1
    parts = len(pieces)
    return pl.pallas_call(
        functools.partial(first_kernel, slots, parts),
        out_shape=[
            jax.ShapeDtypeStruct((blocks * tile, width), jnp.bfloat16),
            jax.ShapeDtypeStruct((8, width), jnp.float32),
        ],
        grid_spec=pltpu.PrefetchScalarGridSpec(
            num_scalar_prefetch=1,
            grid=(blocks // per,),
            in_specs=[pl.BlockSpec((per, slots, tile, tile), lambda i, c: (i, 0, 0, 0))]
            + [pl.BlockSpec(memory_space=pl.ANY)] * parts,
            out_specs=[
                pl.BlockSpec((per * tile, width), lambda i, c: (i, 0)),
                pl.BlockSpec((8, width), lambda i, c: (0, 0)),
            ],
            scratch_shapes=[
                pltpu.VMEM((parts, owners, size, width), jnp.bfloat16),
                pltpu.SemaphoreType.DMA((parts,)),
            ],
        ),
        compiler_params=pltpu.CompilerParams(vmem_limit_bytes=VMEM_LIMIT),
        name="first_product",
    )(columns, tiles, *pieces)


def mix_kernel(mean_ref, p_ref, prior_ref, out_ref):
    groups, _, width = p_ref.shape
    for group in range(groups):
        part = slice(group * width, (group + 1) * width)
        mixed = mixing * p_ref[group].astype(jnp.float32) + (1.0 - mixing) * prior_ref[:, part]
        out_ref[:, part] = (mixed / mean_ref[0]).astype(out_ref.dtype)


def mix(mean, returned, prior, start, dtype):
    groups, rows, width = returned.shape
    size = rows // divisor(rows, rows // 64, 16) if rows > 64 else rows
    if start % size:
        size = 16
    first = start // size
    return pl.pallas_call(
        mix_kernel,
        out_shape=jax.ShapeDtypeStruct((rows, prior.shape[1]), dtype),
        grid=(rows // size,),
        in_specs=[
            pl.BlockSpec(memory_space=pltpu.SMEM),
            pl.BlockSpec((groups, size, width), lambda i: (0, i, 0)),
            pl.BlockSpec((size, prior.shape[1]), lambda i: (i + first, 0)),
        ],
        out_specs=pl.BlockSpec((size, prior.shape[1]), lambda i: (i, 0)),
        compiler_params=pltpu.CompilerParams(vmem_limit_bytes=VMEM_LIMIT),
        name="mix",
    )(mean, returned, prior)


def local(prior, tiles_first, columns_first, tiles_second, columns_second):
    row_count, col_count = lax.axis_size("row"), lax.axis_size("col")
    rows, width = prior.shape
    tile = tiles_first.shape[2]
    cells = float(rows * row_count * width * col_count)
    slab = width // row_count
    aligned = slab % 128 == 0
    groups = row_count if aligned else 1
    chunks = divisor(rows, CHUNKS, tile)
    size = rows // chunks

    all_first = lax.all_gather(tiles_first, "row", axis=0, tiled=True)
    all_columns = lax.all_gather(columns_first, "row", axis=0, tiled=True).reshape(-1)
    inverse_second = 1.0 / jnp.sum(tiles_second, axis=(1, 3), dtype=jnp.float32)[:, None, :]
    turned = tiles_second.transpose(0, 1, 3, 2)
    columns_second = columns_second.reshape(-1)
    prior_part = jnp.sum(prior)

    def product(gathered):
        mixed = second_product(gathered, turned, columns_second, inverse_second, groups)
        if not aligned:
            mixed = mixed.reshape(size, row_count, slab).transpose(1, 0, 2)
        return mixed

    def widen(returned):
        if not aligned:
            returned = returned.transpose(1, 0, 2).reshape(1, -1, width)
        return returned

    ident = 0
    propagated = mean = prior_sum = None
    for iteration in range(ITERS):
        state, ready, pieces = {}, {}, {}
        if iteration == 0:
            state = {
                k: lax.slice_in_dim(prior, k * size, (k + 1) * size).astype(jnp.bfloat16) for k in range(chunks)
            }
        for time in range(0 if iteration else 1, chunks + 2):
            tasks, sources, where = [], [], []
            if iteration and time < chunks:
                tasks.append(("swap", time * size, size))
                sources.append(propagated)
                where.append(("back", time))
            if 0 <= time - 1 < chunks:
                tasks.append(("gather",))
                sources.append(state[time - 1])
                where.append(("gather", time - 1))
            if 0 <= time - 2 < chunks:
                tasks.append(("swap", 0, size))
                sources.append(ready[time - 2])
                where.append(("on", time - 2))
            results = communicate(tuple(tasks), sources, ident)
            ident += 1
            for (kind, k), result in zip(where, results):
                if kind == "back":
                    state[k] = mix(mean, widen(result), prior, k * size, jnp.bfloat16)
                elif kind == "gather":
                    ready[k] = product(result)
                else:
                    pieces[k] = result
        propagated, part = first_product([pieces[k] for k in range(chunks)], all_first, all_columns)
        propagated = propagated.reshape(row_count, rows, slab)
        part = jnp.sum(part)
        if iteration == 0:
            slab_sum, prior_sum = lax.psum((part, prior_part), ("row", "col"))
        else:
            slab_sum = lax.psum(part, ("row", "col"))
        mean = ((mixing * slab_sum + (1.0 - mixing) * prior_sum) / cells).reshape(1)
    (returned,) = communicate((("swap", 0, rows),), [propagated], ident)
    return mix(mean, widen(returned), prior, 0, jnp.float32)


def solution(mesh):
    return jax.shard_map(
        local,
        mesh=mesh,
        in_specs=(
            P("row", "col"),
            P("row", None, None, None),
            P("row", None),
            P("col", None, None, None),
            P("col", None),
        ),
        out_specs=P("row", "col"),
        check_vma=False,
    )
```
